32 devices in a mesh: dp: 2 (over z, core), ep: 16 (over x, y).
Axes of the slice: x: 4, y: 4, z: 1, core: 2. Of those that a mesh axis runs over, the one named last changes fastest.
The devices are a block of a 4x4x8 slice.
Arguments:
- x: bfloat16 [2, 16, 512, 1280], P('dp', 'ep'), parts along dimension 0
- expert: int32 [2, 16, 512, 1], P('dp', 'ep'), parts along dimension 0
- slot: int32 [2, 16, 512, 1], P('dp', 'ep'), parts along dimension 0
- gate: float32 [2, 16, 512, 1], P('dp', 'ep'), parts along dimension 0
- w_gate: bfloat16 [32, 1280, 8192], P('ep')
- w_up: bfloat16 [32, 1280, 8192], P('ep')
- w_down: bfloat16 [32, 8192, 1280], P('ep')
- s_gate: bfloat16 [1280, 8192], replicated
- s_up: bfloat16 [1280, 8192], replicated
- s_down: bfloat16 [8192, 1280], replicated
Outputs:
- y: bfloat16 [2, 16, 512, 1280], P('dp', 'ep'), parts along dimension 0
There are 2 independent parts. The reference program is written for one: setup_inputs(seed, part) draws one part's arguments, and reference() takes and returns one part's arrays. A program takes and returns all parts, laid end to end along the dimension named above; an argument that names none is the same for every part.
All inputs are finite; a program needn't handle non-finite values.
Results may differ from the reference program's by a relative error of at most 0.009.
Values are sent between devices in bfloat16 or wider.
A program may use at most 768 MiB of HBM per device.

```python
import jax
import jax.numpy as jnp

MEMBERS = 16
TOKENS = 512
D = 1280
FF = 8192
TOP = 1
EXPERTS = 32
SHARED_FF = 8192
SLOTS = 5 * TOKENS * TOP // (4 * EXPERTS)


def setup_inputs(seed: int = 0, part: int = 0) -> dict:
    own, k1, k2, k3, k4, k5, k6 = jax.random.split(jax.random.key(seed), 7)
    kx, ke, kl, kg = jax.random.split(jax.random.fold_in(own, part), 4)
    devices = (1, MEMBERS)
    place = jax.random.permutation(kl, jnp.arange(EXPERTS, dtype=jnp.uint32))
    slow = ((EXPERTS + (9 * place) % EXPERTS) << ((9 * place) // EXPERTS)) // EXPERTS
    wait = (jax.random.bits(ke, (*devices, TOKENS, EXPERTS), jnp.uint32) >> 10) * slow
    expert = jnp.argsort(wait, axis=-1)[..., :TOP].astype(jnp.int32)
    chosen = jax.nn.one_hot(expert, EXPERTS, dtype=jnp.int32)
    in_line = jnp.cumsum(chosen.reshape(*devices, TOKENS * TOP, EXPERTS), axis=2) - 1
    slot = jnp.sum(in_line.reshape(chosen.shape) * chosen, axis=-1)

    def one(key, rows, columns):
        return (jax.random.normal(key, (rows, columns), jnp.float32) * rows**-0.5).astype(jnp.bfloat16)

    def weights(key, rows, columns):
        return jax.lax.map(lambda k: one(k, rows, columns), jax.random.split(key, EXPERTS))

    return {
        "x": jax.random.normal(kx, (*devices, TOKENS, D), jnp.float32).astype(jnp.bfloat16),
        "expert": expert,
        "slot": slot,
        "gate": jax.nn.sigmoid(jax.random.normal(kg, expert.shape, jnp.float32)),
        "w_gate": weights(k1, D, FF),
        "w_up": weights(k2, D, FF),
        "w_down": weights(k3, FF, D),
        "s_gate": one(k4, D, SHARED_FF),
        "s_up": one(k5, D, SHARED_FF),
        "s_down": one(k6, SHARED_FF, D),
    }


def einsum(form, a, b):
    return jnp.einsum(form, a.astype(jnp.float32), b.astype(jnp.float32))


def for_all(x, s_gate, s_up, s_down):
    h = jax.nn.silu(einsum("...d,df->...f", x, s_gate)) * einsum("...d,df->...f", x, s_up)
    return einsum("...f,fd->...d", h.astype(jnp.bfloat16), s_down)


def reference(x, expert, slot, gate, w_gate, w_up, w_down, s_gate, s_up, s_down):
    to_expert = jax.nn.one_hot(expert, EXPERTS, dtype=jnp.bfloat16)
    to_slot = jax.nn.one_hot(slot, SLOTS, dtype=jnp.bfloat16)
    weighted = to_expert * gate[..., None].astype(jnp.bfloat16)
    dispatch = einsum("abtke,abtkc->abtec", to_expert, to_slot).astype(jnp.bfloat16)
    combine = einsum("abtke,abtkc->abtec", weighted, to_slot).astype(jnp.bfloat16)
    z = einsum("abtec,abtd->aebcd", dispatch, x).astype(jnp.bfloat16)
    h = jax.nn.silu(einsum("aebcd,edf->aebcf", z, w_gate))
    h = (h * einsum("aebcd,edf->aebcf", z, w_up)).astype(jnp.bfloat16)
    out = einsum("aebcf,efd->aebcd", h, w_down).astype(jnp.bfloat16)
    y = einsum("abtec,aebcd->abtd", combine, out)
    return (y + for_all(x, s_gate, s_up, s_down)).astype(jnp.bfloat16)
```

```python
import functools

import jax
import jax.numpy as jnp
from jax import lax
from jax.experimental import pallas as pl
from jax.experimental.pallas import tpu as pltpu
from jax.sharding import PartitionSpec as P

F32, BF16 = jnp.float32, jnp.bfloat16
TILE = 512
UNROLL = 4
RING = 10
LEAD = 8
COL = 256


def kernel(
    n, slots, steps,
    x_hbm, expert, slot, gate, wg, wu, wd, sg, su, sd, y_hbm,
    x_v, zsend, zrecv, z_v, osend, orecv, acc_s, acc_r, h0, h1, bg, bu, bd,
    x_sem, w_sem, zs_sem, zr_sem, os_sem, or_sem, y_sem,
):
    me = lax.axis_index("ep")
    tokens, width = x_v.shape
    local = wg.shape[0]
    block = zsend.shape[2]
    routed = local * steps
    total = routed + steps
    parity = lax.rem(me, 2)

    barrier = pltpu.get_barrier_semaphore()

    def greet(o, c):
        pl.semaphore_signal(barrier, inc=1, device_id={"ep": lax.rem(me + o, n)})
        return c

    lax.fori_loop(1, n, greet, 0)
    x_copy = pltpu.make_async_copy(x_hbm, x_v, x_sem)
    x_copy.start()

    def copies(at, gate_w, up_w, down_w, column):
        cols = pl.ds(pl.multiple_of(column * TILE, TILE), TILE)
        return (
            pltpu.make_async_copy(gate_w.at[:, cols], bg.at[at], w_sem.at[at, 0]),
            pltpu.make_async_copy(up_w.at[:, cols], bu.at[at], w_sem.at[at, 1]),
            pltpu.make_async_copy(down_w.at[cols, :], bd.at[at], w_sem.at[at, 2]),
        )

    def fetch(s):
        at = lax.rem(s, RING)
        before, after = s < LEAD, s >= LEAD + routed

        @pl.when(jnp.logical_and(jnp.logical_or(before, after), s < total))
        def _():
            column = jnp.where(before, s, s - routed)
            for c in copies(at, sg, su, sd, column):
                c.start()

        @pl.when(jnp.logical_not(jnp.logical_or(before, after)))
        def _():
            r = s - LEAD
            e = r // steps
            for c in copies(at, wg.at[e], wu.at[e], wd.at[e], lax.rem(r, steps)):
                c.start()

    def prefill(s, c):
        fetch(s)
        return c

    lax.fori_loop(0, RING - UNROLL, prefill, 0)

    def target():
        e, s = expert[...], slot[...]
        row = lax.rem(e, local) * (n * block) + (e // local) * block + s + 4 * parity
        return jnp.where(s < slots, row, -1)

    def dispatch(j):
        rows = lax.broadcasted_iota(jnp.int32, (n * block, tokens), 0) + j * (n * block)
        pick = jnp.where(rows == target(), 1.0, 0.0).astype(BF16)
        z = jnp.dot(pick, x_v[...], preferred_element_type=F32)
        for d in range(n):
            zsend[j, d] = z[d * block : (d + 1) * block].astype(BF16)

    def exchange(j, o, src, dst, s_sem, r_sem):
        to = lax.rem(me + o, n)
        return pltpu.make_async_remote_copy(
            src_ref=src.at[j, to],
            dst_ref=dst.at[j, me],
            send_sem=s_sem.at[j, o],
            recv_sem=r_sem.at[j, o],
            device_id={"ep": to},
        )

    def arrive(j, o, src, dst, s_sem, r_sem):
        frm = lax.rem(me + n - o, n)
        return pltpu.make_async_remote_copy(
            src_ref=src.at[j, frm],
            dst_ref=dst.at[j, frm],
            send_sem=s_sem.at[j, o],
            recv_sem=r_sem.at[j, o],
            device_id={"ep": frm},
        )

    def send_all(j, *refs):
        def one(o, c):
            exchange(j, o, *refs).start()
            return c

        lax.fori_loop(1, n, one, 0)
        src, dst = refs[:2]
        dst[j, me] = src[j, me]

    def wait_all(j, *refs):
        def one(o, c):
            arrive(j, o, *refs).wait_recv()
            return c

        lax.fori_loop(1, n, one, 0)

    def sent_all(j, *refs):
        def one(o, c):
            exchange(j, o, *refs).wait_send()
            return c

        lax.fori_loop(1, n, one, 0)

    z_refs = (zsend, zrecv, zs_sem, zr_sem)
    o_refs = (osend, orecv, os_sem, or_sem)

    x_copy.wait()
    for j in range(local):
        dispatch(j)
    pl.semaphore_wait(barrier, n - 1)
    for j in range(local):
        send_all(j, *z_refs)

    hs = (h0, h1)

    def run(base, rows, lhs, acc):
        ats = [lax.rem(base + k, RING) for k in range(UNROLL)]
        for k in range(UNROLL):
            for c in copies(ats[k], sg, su, sd, 0):
                c.wait()
        for k in range(UNROLL):
            fetch(base + (RING - UNROLL) + k)
        for k in range(UNROLL + 1):
            if k < UNROLL:
                h = hs[k % 2]
                for a in range(0, TILE, COL):
                    g = jnp.dot(lhs[...], bg[ats[k], :, a : a + COL], preferred_element_type=F32)
                    u = jnp.dot(lhs[...], bu[ats[k], :, a : a + COL], preferred_element_type=F32)
                    h[:rows, a : a + COL] = (jax.nn.silu(g) * u).astype(BF16)
            if k > 0:
                h = hs[(k - 1) % 2]
                for a in range(0, width, COL):
                    acc[:, a : a + COL] += jnp.dot(
                        h[:rows, :], bd[ats[k - 1], :, a : a + COL], preferred_element_type=F32
                    )

    def shared(i, c):
        run(i * UNROLL, tokens, x_v, acc_s)
        return c

    acc_s[...] = jnp.zeros_like(acc_s)
    lax.fori_loop(0, LEAD // UNROLL, shared, 0)

    rows = n * slots

    def one_expert(j, c):
        wait_all(j, *z_refs)
        for q in range(0, n, 4):
            parts = []
            for p in (q, q + 2):
                even, odd = zrecv[j, p].astype(F32), zrecv[j, p + 1].astype(F32)
                parts += [even[:16], even[16:] + odd[:8], odd[8:]]
            z_v[q * slots : (q + 4) * slots, :] = jnp.concatenate(parts, axis=0).astype(BF16)
        acc_r[...] = jnp.zeros_like(acc_r)

        def part(i, c):
            run(LEAD + j * steps + i * UNROLL, rows, z_v, acc_r)
            return c

        lax.fori_loop(0, steps // UNROLL, part, 0)
        for d in range(n):
            first = d * slots // 8 * 8
            osend[j, d] = acc_r[first : first + block, :].astype(BF16)
        send_all(j, *o_refs)
        return c

    lax.fori_loop(0, local, one_expert, 0)

    def combine(j):
        wait_all(j, *o_refs)
        at = lax.broadcasted_iota(jnp.int32, (n * block, tokens), 0) + j * (n * block)
        weight = gate[...].astype(BF16).astype(F32)
        pick = jnp.where(at == target(), weight, 0.0).astype(BF16)
        out = jnp.concatenate([orecv[j, d].astype(F32) for d in range(n)], axis=0).astype(BF16)
        return lax.dot_general(pick, out, (((0,), (0,)), ((), ())), preferred_element_type=F32)

    for j in range(local - 1):
        acc_s[...] += combine(j)

    def tail(i, c):
        run(LEAD + routed + i * UNROLL, tokens, x_v, acc_s)
        return c

    lax.fori_loop(0, (steps - LEAD) // UNROLL, tail, 0)

    x_v[...] = (acc_s[...] + combine(local - 1)).astype(BF16)
    y_copy = pltpu.make_async_copy(x_v, y_hbm, y_sem)
    y_copy.start()
    for j in range(local):
        sent_all(j, *z_refs)
        sent_all(j, *o_refs)
    y_copy.wait()


def solution(mesh):
    n = mesh.shape["ep"]

    def part(x, expert, slot, gate, wg, wu, wd, sg, su, sd):
        tokens, width = x.shape[2:]
        local, _, hidden = wg.shape
        slots = 5 * tokens * expert.shape[-1] // (4 * local * n)
        block = slots + 4
        assert slots % 8 == 4 and hidden == sg.shape[1]
        steps = hidden // TILE
        hbm = pl.BlockSpec(memory_space=pl.ANY)
        vmem = pl.BlockSpec(memory_space=pltpu.VMEM)
        flops = 6 * width * hidden * (tokens + local * n * slots)
        y = pl.pallas_call(
            functools.partial(kernel, n, slots, steps),
            out_shape=jax.ShapeDtypeStruct((tokens, width), BF16),
            in_specs=[hbm, vmem, vmem, vmem] + [hbm] * 6,
            out_specs=hbm,
            scratch_shapes=[
                pltpu.VMEM((tokens, width), BF16),
                pltpu.VMEM((local, n, block, width), BF16),
                pltpu.VMEM((local, n, block, width), BF16),
                pltpu.VMEM((n * slots, width), BF16),
                pltpu.VMEM((local, n, block, width), BF16),
                pltpu.VMEM((local, n, block, width), BF16),
                pltpu.VMEM((tokens, width), F32),
                pltpu.VMEM((n * slots, width), F32),
                pltpu.VMEM((tokens, TILE), BF16),
                pltpu.VMEM((tokens, TILE), BF16),
                pltpu.VMEM((RING, width, TILE), BF16),
                pltpu.VMEM((RING, width, TILE), BF16),
                pltpu.VMEM((RING, TILE, width), BF16),
                pltpu.SemaphoreType.DMA,
                pltpu.SemaphoreType.DMA((RING, 3)),
                pltpu.SemaphoreType.DMA((local, n)),
                pltpu.SemaphoreType.DMA((local, n)),
                pltpu.SemaphoreType.DMA((local, n)),
                pltpu.SemaphoreType.DMA((local, n)),
                pltpu.SemaphoreType.DMA,
            ],
            compiler_params=pltpu.CompilerParams(
                collective_id=0, has_side_effects=True, vmem_limit_bytes=67043328
            ),
            cost_estimate=pl.CostEstimate(flops=flops, bytes_accessed=6 * width * hidden * (1 + local), transcendentals=0),
            name="moe",
        )(
            x.reshape(tokens, width),
            expert.reshape(1, tokens),
            slot.reshape(1, tokens),
            gate.reshape(1, tokens),
            wg, wu, wd, sg, su, sd,
        )
        return y.reshape(x.shape)

    a, e, s = P("dp", "ep"), P("ep"), P()
    return jax.shard_map(
        part,
        mesh=mesh,
        in_specs=(a, a, a, a, e, e, e, s, s, s),
        out_specs=a,
        check_vma=False,
    )
```

```python
import functools
import math

import jax
import jax.numpy as jnp
from jax import lax
from jax.experimental import pallas as pl
from jax.experimental.pallas import tpu as pltpu
from jax.sharding import PartitionSpec as P

F32, BF16 = jnp.float32, jnp.bfloat16
TILE = 512
SHORT, LONG = 2, 4
RING = 10
LEAD = 8
COL = 256
VMEM = 62 << 20


def ahead(step, ring):
    return step if 2 * step <= ring else 0


def kernel(
    n, slots, steps,
    x_hbm, expert, slot, gate, wg, wu, wd, sg, su, sd, y_hbm,
    x_v, zsend, zrecv, z_v, osend, orecv, acc_s, acc_r, h0, h1, bg, bu, bd,
    x_sem, w_sem, zs_sem, zr_sem, os_sem, or_sem, y_sem,
):
    me = lax.axis_index("ep")
    tokens, width = x_v.shape
    local = wg.shape[0]
    block = zsend.shape[2]
    routed = local * steps
    total = routed + steps
    parity = lax.rem(me, 2)

    barrier = pltpu.get_barrier_semaphore()

    def greet(o, c):
        pl.semaphore_signal(barrier, inc=1, device_id={"ep": lax.rem(me + o, n)})
        return c

    lax.fori_loop(1, n, greet, 0)
    x_copy = pltpu.make_async_copy(x_hbm, x_v, x_sem)
    x_copy.start()

    def copies(at, gate_w, up_w, down_w, column):
        cols = pl.ds(pl.multiple_of(column * TILE, TILE), TILE)
        return (
            pltpu.make_async_copy(gate_w.at[:, cols], bg.at[at], w_sem.at[at, 0]),
            pltpu.make_async_copy(up_w.at[:, cols], bu.at[at], w_sem.at[at, 1]),
            pltpu.make_async_copy(down_w.at[cols, :], bd.at[at], w_sem.at[at, 2]),
        )

    def fetch(s):
        at = lax.rem(s, RING)
        before, after = s < LEAD, s >= LEAD + routed

        @pl.when(jnp.logical_and(jnp.logical_or(before, after), s < total))
        def _():
            column = jnp.where(before, s, s - routed)
            for c in copies(at, sg, su, sd, column):
                c.start()

        @pl.when(jnp.logical_not(jnp.logical_or(before, after)))
        def _():
            r = s - LEAD
            e = r // steps
            for c in copies(at, wg.at[e], wu.at[e], wd.at[e], lax.rem(r, steps)):
                c.start()

    def prefill(s, c):
        fetch(s)
        return c

    lax.fori_loop(0, RING, prefill, 0)

    def target():
        e, s = expert[...], slot[...]
        row = lax.rem(e, local) * (n * block) + (e // local) * block + s + 4 * parity
        return jnp.where(s < slots, row, -1)

    def dispatch(j):
        rows = lax.broadcasted_iota(jnp.int32, (n * block, tokens), 0) + j * (n * block)
        pick = jnp.where(rows == target(), 1.0, 0.0).astype(BF16)
        z = jnp.dot(pick, x_v[...], preferred_element_type=F32)
        for d in range(n):
            zsend[j, d] = z[d * block : (d + 1) * block].astype(BF16)

    side = math.isqrt(n)
    side = side if side * side == n else 1
    far = sorted(range(1, n), key=lambda o: (-ahead(o // side, n // side) - ahead(o % side, side), o))

    def peer(o, sign):
        i = lax.rem(me // side + n // side + sign * (o // side), n // side)
        return i * side + lax.rem(lax.rem(me, side) + side + sign * (o % side), side)

    def exchange(j, o, src, dst, s_sem, r_sem):
        to = peer(o, 1)
        return pltpu.make_async_remote_copy(
            src_ref=src.at[j, to],
            dst_ref=dst.at[j, me],
            send_sem=s_sem.at[j, o],
            recv_sem=r_sem.at[j, o],
            device_id={"ep": to},
        )

    def arrive(j, o, src, dst, s_sem, r_sem):
        frm = peer(o, -1)
        return pltpu.make_async_remote_copy(
            src_ref=src.at[j, frm],
            dst_ref=dst.at[j, frm],
            send_sem=s_sem.at[j, o],
            recv_sem=r_sem.at[j, o],
            device_id={"ep": frm},
        )

    def send_all(j, *refs):
        for o in far:
            exchange(j, o, *refs).start()
        src, dst = refs[:2]
        dst[j, me] = src[j, me]

    def wait_all(j, *refs):
        for o in far:
            arrive(j, o, *refs).wait_recv()

    def sent_all(j, *refs):
        for o in far:
            exchange(j, o, *refs).wait_send()

    z_refs = (zsend, zrecv, zs_sem, zr_sem)
    o_refs = (osend, orecv, os_sem, or_sem)

    x_copy.wait()
    dispatch(0)

    hs = (h0, h1)

    def run(base, count, freed, rows, lhs, acc):
        ats = [lax.rem(base + k, RING) for k in range(count)]
        lax.fori_loop(base + RING - freed, base + RING, prefill, 0)
        for k in range(count):
            for c in copies(ats[k], sg, su, sd, 0):
                c.wait()
        for k in range(count + 1):
            if k < count:
                h = hs[k % 2]
                for a in range(0, TILE, COL):
                    g = jnp.dot(lhs[...], bg[ats[k], :, a : a + COL], preferred_element_type=F32)
                    u = jnp.dot(lhs[...], bu[ats[k], :, a : a + COL], preferred_element_type=F32)
                    h[:rows, a : a + COL] = (jax.nn.silu(g) * u).astype(BF16)
            if k > 0:
                h = hs[(k - 1) % 2]
                for a in range(0, width, COL):
                    acc[:, a : a + COL] += jnp.dot(
                        h[:rows, :], bd[ats[k - 1], :, a : a + COL], preferred_element_type=F32
                    )

    def shared(i, c):
        run(2 + i * SHORT, SHORT, jnp.where(i == 0, 1, SHORT), tokens, x_v, acc_s)
        return c

    acc_s[...] = jnp.zeros_like(acc_s)
    run(0, 1, 0, tokens, x_v, acc_s)
    pl.semaphore_wait(barrier, n - 1)
    send_all(0, *z_refs)
    for j in range(1, local):
        dispatch(j)
    run(1, 1, 1, tokens, x_v, acc_s)
    lax.fori_loop(0, (LEAD - 2) // SHORT, shared, 0)

    rows = n * slots

    def one_expert(j, c):
        wait_all(j, *z_refs)

        @pl.when(j + 1 < local)
        def _():
            send_all(j + 1, *z_refs)

        for q in range(0, n, 4):
            parts = []
            for p in (q, q + 2):
                even, odd = zrecv[j, p].astype(F32), zrecv[j, p + 1].astype(F32)
                parts += [even[:16], even[16:] + odd[:8], odd[8:]]
            z_v[q * slots : (q + 4) * slots, :] = jnp.concatenate(parts, axis=0).astype(BF16)
        acc_r[...] = jnp.zeros_like(acc_r)

        def part(i, c):
            freed = jnp.where(jnp.logical_and(i == 0, j == 0), SHORT, LONG)
            run(LEAD + j * steps + i * LONG, LONG, freed, rows, z_v, acc_r)
            return c

        lax.fori_loop(0, steps // LONG, part, 0)
        for d in range(n):
            first = d * slots // 8 * 8
            osend[j, d] = acc_r[first : first + block, :].astype(BF16)
        send_all(j, *o_refs)
        return c

    lax.fori_loop(0, local, one_expert, 0)

    def returned(j):
        wait_all(j, *o_refs)
        return jnp.concatenate([orecv[j, d].astype(F32) for d in range(n)], axis=0).astype(BF16)

    def combine(j, out, cols):
        at = lax.broadcasted_iota(jnp.int32, (n * block, tokens), 0) + j * (n * block)
        weight = gate[...].astype(BF16).astype(F32)
        pick = jnp.where(at == target(), weight, 0.0).astype(BF16)[:, cols]
        return lax.dot_general(pick, out, (((0,), (0,)), ((), ())), preferred_element_type=F32)

    for j in range(local - 1):
        acc_s[...] += combine(j, returned(j), slice(None))

    def tail(i, c):
        run(LEAD + routed + i * LONG, LONG, LONG, tokens, x_v, acc_s)
        return c

    lax.fori_loop(0, (steps - LEAD) // LONG, tail, 0)

    last, half, y_copies = returned(local - 1), tokens // 2, []
    for i in range(2):
        part = slice(i * half, (i + 1) * half)
        x_v[part, :] = (acc_s[part, :] + combine(local - 1, last, part)).astype(BF16)
        y_copies.append(pltpu.make_async_copy(x_v.at[part], y_hbm.at[part], y_sem.at[i]))
        y_copies[i].start()
    for j in range(local):
        sent_all(j, *z_refs)
        sent_all(j, *o_refs)
    for c in y_copies:
        c.wait()


def solution(mesh):
    n = mesh.shape["ep"]

    def part(x, expert, slot, gate, wg, wu, wd, sg, su, sd):
        tokens, width = x.shape[2:]
        local, _, hidden = wg.shape
        slots = 5 * tokens * expert.shape[-1] // (4 * local * n)
        block = slots + 4
        assert slots % 8 == 4 and hidden == sg.shape[1]
        steps = hidden // TILE
        hbm = pl.BlockSpec(memory_space=pl.ANY)
        vmem = pl.BlockSpec(memory_space=pltpu.VMEM)
        flops = 6 * width * hidden * (tokens + local * n * slots)
        y = pl.pallas_call(
            functools.partial(kernel, n, slots, steps),
            out_shape=jax.ShapeDtypeStruct((tokens, width), BF16),
            in_specs=[hbm, vmem, vmem, vmem] + [hbm] * 6,
            out_specs=hbm,
            scratch_shapes=[
                pltpu.VMEM((tokens, width), BF16),
                pltpu.VMEM((local, n, block, width), BF16),
                pltpu.VMEM((local, n, block, width), BF16),
                pltpu.VMEM((n * slots, width), BF16),
                pltpu.VMEM((local, n, block, width), BF16),
                pltpu.VMEM((local, n, block, width), BF16),
                pltpu.VMEM((tokens, width), F32),
                pltpu.VMEM((n * slots, width), F32),
                pltpu.VMEM((tokens, TILE), BF16),
                pltpu.VMEM((tokens, TILE), BF16),
                pltpu.VMEM((RING, width, TILE), BF16),
                pltpu.VMEM((RING, width, TILE), BF16),
                pltpu.VMEM((RING, TILE, width), BF16),
                pltpu.SemaphoreType.DMA,
                pltpu.SemaphoreType.DMA((RING, 3)),
                pltpu.SemaphoreType.DMA((local, n)),
                pltpu.SemaphoreType.DMA((local, n)),
                pltpu.SemaphoreType.DMA((local, n)),
                pltpu.SemaphoreType.DMA((local, n)),
                pltpu.SemaphoreType.DMA((2,)),
            ],
            compiler_params=pltpu.CompilerParams(
                collective_id=0, has_side_effects=True, vmem_limit_bytes=VMEM
            ),
            cost_estimate=pl.CostEstimate(flops=flops, bytes_accessed=6 * width * hidden * (1 + local), transcendentals=0),
            name="moe",
        )(
            x.reshape(tokens, width),
            expert.reshape(1, tokens),
            slot.reshape(1, tokens),
            gate.reshape(1, tokens),
            wg, wu, wd, sg, su, sd,
        )
        return y.reshape(x.shape)

    a, e, s = P("dp", "ep"), P("ep"), P()
    return jax.shard_map(
        part,
        mesh=mesh,
        in_specs=(a, a, a, a, e, e, e, s, s, s),
        out_specs=a,
        check_vma=False,
    )
```
